32 devices in a mesh: grp: 16 (over z, y, core), seq: 2 (over x).
Axes of the slice: x: 2, y: 2, z: 4, core: 2. Of those that a mesh axis runs over, the one named last changes fastest.
Arguments:
- queries: bfloat16 [8192, 4096], P(('grp', 'seq')), may hold values from -8 to 8
- keys: bfloat16 [8192, 4096], P(('grp', 'seq')), may hold values from -6 to 6
- values: bfloat16 [8192, 4096], P(('grp', 'seq')), may hold values from -6 to 6
- global_pos: int32 [64], P(('grp', 'seq')), may hold values from 0 to 127
- layout: int32 [64, 32], P(('grp', 'seq')), may hold values from 0 to 63, all different within a row
Outputs:
- attended: bfloat16 [8192, 4096], P(('grp', 'seq'))
The draws below stay inside these ranges and needn't reach their ends.
Inputs may be any that keep to these rules, and one draw needn't show every extreme that they name: `layout`: each row lists 32 different block indices, and every block is listed by some row.
All inputs are finite; a program needn't handle non-finite values.
Results may differ from the reference program's by a relative error of at most 0.0042.
Values may be sent and summed in bfloat16 or wider, within the bound.
A program may use at most 128 MiB of HBM per device.

```python
import math
import jax
import jax.numpy as jnp
from jax import lax

HEADS = 32
HEAD_DIM = 128
BLOCK = 128
LINKS = 32
WIDTH = 4096
SEQ = 8192
NBLK = 64


def draw_queries(key, part):
    base = jnp.clip(2.0 * jax.random.normal(jax.random.fold_in(key, 1), (SEQ, HEADS * HEAD_DIM), jnp.float32), -8.0, 8.0)
    return base.astype(jnp.bfloat16)


def draw_keys(key, part):
    base = jnp.clip(jax.random.normal(jax.random.fold_in(key, 2), (SEQ, HEADS * HEAD_DIM), jnp.float32), -6.0, 6.0)
    return base.astype(jnp.bfloat16)


def with_ends(entries, key, smallest, largest):
    longest = entries.shape.index(max(entries.shape))
    spots = []
    for shift in (0, 1):
        where = [jax.random.randint(jax.random.fold_in(key, axis), (), 0, length) for axis, length in enumerate(entries.shape)]
        where[longest] = (where[longest] + shift) % entries.shape[longest]
        spots.append(tuple(where))
    return entries.at[spots[0]].set(smallest).at[spots[1]].set(largest)


def shard_levels(key, extent, pieces, smallest, high):
    def one(dim, shards_of):
        heights = jax.random.uniform(jax.random.fold_in(jax.random.fold_in(key, 6), dim), (shards_of,), jnp.float32, smallest / len(pieces), high / len(pieces))
        return jnp.repeat(jnp.exp(heights), extent[dim] // shards_of).reshape((-1,) + (1,) * (len(extent) - dim - 1))

    factor_of = one(*pieces[0])
    for cut in pieces[1:]:
        factor_of = factor_of * one(*cut)
    return factor_of


def picks_of(key, rows, amount, top, lift):
    sequence = jax.random.permutation(jax.random.fold_in(key, 1), amount)
    boost = sequence
    for power in range(3):
        boost = boost * boost // amount
    boost = boost * lift // amount
    lots = jax.random.randint(jax.random.fold_in(key, 2), (rows, amount), 0, 4096) + boost
    sure = jax.random.permutation(jax.random.fold_in(key, 3), rows)[jnp.arange(amount) % rows]
    lots = jnp.where(jnp.arange(rows)[:, None] == sure[None, :], 1 << 14, lots)
    merit = lots * amount + jnp.arange(amount)
    return lax.top_k(merit.astype(jnp.int32), top)[1].astype(jnp.int32)


def noise(rng, dims, scale, reach, split=(), kind=jnp.bfloat16):
    values = jax.random.normal(rng, dims, jnp.float32) * scale
    if len(split) > 0:
        values = shard_levels(rng, dims, split, -0.22, 0.18) * values
    return jnp.clip(values, min=-reach, max=reach).astype(kind)


def setup_inputs(seed: int = 0) -> dict:
    seeds = jax.random.split(jax.random.key(seed), 6)
    return {
        "queries": draw_queries(jax.random.fold_in(seeds[5], 71), 0),
        "keys": draw_keys(jax.random.fold_in(seeds[5], 71), 0),
        "values": noise(seeds[2], (SEQ, WIDTH), 1.0, 6.0, ((0, 32),)),
        "global_pos": with_ends(jax.random.randint(seeds[3], (NBLK,), 0, BLOCK), jax.random.fold_in(seeds[3], 1), 0, BLOCK - 1).astype(jnp.int32),
        "layout": picks_of(seeds[4], NBLK, NBLK, LINKS, 0),
    }


def pooled(source, blocks_all):
    blocks = source.astype(jnp.float32).reshape(blocks_all, BLOCK, HEADS, HEAD_DIM).mean(axis=1)
    spread = lax.optimization_barrier(jnp.mean(blocks * blocks, axis=-1, keepdims=True))
    return (blocks / jnp.sqrt(spread + 1e-06)).reshape(blocks_all, HEADS * HEAD_DIM).astype(jnp.bfloat16)

def reference(queries, keys, values, global_pos, layout):
    score_scale = 1.0 / math.sqrt(HEAD_DIM)
    summary_keys = pooled(keys, NBLK).astype(jnp.float32).reshape(NBLK, HEADS, HEAD_DIM)
    summary_values = pooled(values, NBLK).astype(jnp.float32).reshape(NBLK, HEADS, HEAD_DIM)
    padding = jnp.zeros((BLOCK, HEADS * HEAD_DIM), jnp.bfloat16)
    padded_keys = jnp.concatenate([padding, keys, padding], axis=0)
    padded_values = jnp.concatenate([padding, values, padding], axis=0)
    block_ids = jnp.arange(NBLK, dtype=jnp.int32)

    def one_block(which):
        first_row = (which * BLOCK).astype(jnp.int32)
        query_rows = lax.dynamic_slice_in_dim(queries, first_row, BLOCK, 0).astype(jnp.float32).reshape(BLOCK, HEADS, HEAD_DIM)
        window_keys = lax.dynamic_slice_in_dim(padded_keys, first_row, 3 * BLOCK, 0).astype(jnp.float32).reshape(3 * BLOCK, HEADS, HEAD_DIM)
        window_values = lax.dynamic_slice_in_dim(padded_values, first_row, 3 * BLOCK, 0).astype(jnp.float32).reshape(3 * BLOCK, HEADS, HEAD_DIM)
        window_scores = jnp.einsum('qhd,khd->hqk', query_rows, window_keys) * score_scale
        key_block = jnp.arange(3 * BLOCK, dtype=jnp.int32) // BLOCK + which - 1
        inside = (key_block >= 0) & (key_block < NBLK)
        window_scores = jnp.where(inside[None, None, :], window_scores, -jnp.inf)
        summary_scores = jnp.einsum('qhd,jhd->hqj', query_rows, summary_keys) * score_scale
        listed = jnp.any(layout[which][:, None] == block_ids[None, :], axis=0)
        is_global = jnp.arange(BLOCK, dtype=jnp.int32) == global_pos[which]
        visible = listed[None, :] | is_global[:, None]
        summary_scores = jnp.where(visible[None, :, :], summary_scores, -jnp.inf)
        peak = jnp.maximum(lax.optimization_barrier(jnp.max(window_scores, axis=-1)), lax.optimization_barrier(jnp.max(summary_scores, axis=-1)))
        window_weights = jnp.exp(window_scores - peak[..., None])
        summary_weights = jnp.exp(summary_scores - peak[..., None])
        denominator = lax.optimization_barrier(jnp.sum(window_weights, axis=-1)) + lax.optimization_barrier(jnp.sum(summary_weights, axis=-1))
        rounded_window = lax.optimization_barrier(window_weights.astype(jnp.bfloat16)).astype(jnp.float32)
        rounded_summary = lax.optimization_barrier(summary_weights.astype(jnp.bfloat16)).astype(jnp.float32)
        numerator = jnp.einsum('hqk,khd->hqd', rounded_window, window_values)
        numerator = numerator + jnp.einsum('hqj,jhd->hqd', rounded_summary, summary_values)
        result = numerator / denominator[..., None]
        return jnp.transpose(result, (1, 0, 2)).reshape(BLOCK, HEADS * HEAD_DIM).astype(jnp.bfloat16)
    outputs = lax.map(one_block, block_ids)
    return outputs.reshape(SEQ, HEADS * HEAD_DIM)
```

```python
import functools
import math

import jax
import jax.numpy as jnp
from jax import lax
from jax.experimental import pallas as pl
from jax.experimental.pallas import tpu as pltpu
from jax.sharding import PartitionSpec as P

HEAD_DIM = 128
BLOCK = 128
CHUNK_HEADS = 2
EARLY_CHUNKS = 2
PLANE_BITS = 2
POOL_HEADS = 8
MESH = pl.DeviceIdType.MESH


def dot_t(a, b):
    return lax.dot_general(a, b, (((1,), (1,)), ((), ())), preferred_element_type=jnp.float32)


def dot(a, b):
    return jnp.dot(a, b, preferred_element_type=jnp.float32)


def kernel(
    groups, seqs, pos_hbm, layout_hbm, q_hbm, k_hbm, v_hbm, out,
    pos_ref, layout_ref, q, k, v, halo, relay, gathered, own, wide, bias,
    load_sem, send_sem, recv_sem, relay_recv, relay_send, seq_send, seq_recv,
    line_send, line_recv, bit_send, bit_recv,
):
    rows, width = q.shape
    heads = width // HEAD_DIM
    blocks = rows // BLOCK
    devices = groups * seqs
    total_blocks = devices * blocks
    step_cols = CHUNK_HEADS * HEAD_DIM
    chunks = heads // CHUNK_HEADS
    bits, planes = gather_shape(groups)
    low = 1 << bits
    relaying = relays(groups, seqs)

    g, s = lax.axis_index("grp"), lax.axis_index("seq")
    me = g * seqs + s
    has_left, has_right = me > 0, me < devices - 1
    plane, lane = g // low, g % low

    def coords(position):
        return (position // seqs, position % seqs)

    first = s % 2
    second = 1 - first

    def exists(side):
        return jnp.where(side == 0, has_right, has_left)

    def neighbour(side):
        return jnp.clip(me + 1 - 2 * side, 0, devices - 1)

    pairs = groups // 2
    step_pair = 2 * seqs
    far = (g % 2 == s) if relaying else False
    rank = jnp.where(s == 0, g // 2, pairs - 1 - g // 2)
    odd = rank % 2 == 1
    across = me + (step_pair - 1) * (1 - 2 * s)
    behind, ahead = me + step_pair * (1 - 2 * s), me - step_pair * (1 - 2 * s)
    handed = jnp.where(far, chunks * jnp.where(odd, 1, rank) // pairs, 0) if relaying else 0
    via = jnp.where(odd, ahead, across)
    passing = chunks * jnp.where(odd, pairs - 1 - rank, 1) // pairs
    target = jnp.where(odd, behind, across)
    target_side = jnp.where(odd, first, second)

    loads = [
        pltpu.make_async_copy(src, dst, load_sem.at[i])
        for i, (src, dst) in enumerate(((k_hbm, k), (v_hbm, v), (q_hbm, q), (pos_hbm, pos_ref), (layout_hbm, layout_ref)))
    ]
    barrier = pltpu.get_barrier_semaphore()

    peers = [(exists(side), neighbour(side)) for side in range(2)]
    peers += [(True, g * seqs + lax.rem(s + o, seqs)) for o in range(1, seqs)]
    peers += [(True, (g ^ (1 << bit)) * seqs + s) for bit in range(bits)]
    if planes > 1:
        peers += [
            (plane > 0, jnp.maximum(me - low * seqs, 0)),
            (plane < planes - 1, jnp.minimum(me + low * seqs, devices - 1)),
        ]
    if relaying:
        peers += [(far, across), (far & (rank > 0), ahead), (far & (rank < pairs - 1), behind)]
    for load in loads:
        load.start()
    expected = 0
    for there, peer in peers:
        if there is True:
            pl.semaphore_signal(barrier, inc=1, device_id=coords(peer), device_id_type=MESH)
            expected = expected + 1
        else:
            @pl.when(there)
            def _(peer=peer):
                pl.semaphore_signal(barrier, inc=1, device_id=coords(peer), device_id_type=MESH)
            expected = expected + there.astype(jnp.int32)
    pl.semaphore_wait(barrier, expected)

    def columns(c):
        return pl.ds(pl.multiple_of(c * step_cols, step_cols), step_cols)

    def edge(side, kv, c):
        start = pl.multiple_of((rows - BLOCK) * (1 - side), BLOCK)
        return pltpu.make_async_remote_copy(
            src_ref=(k_hbm, v_hbm)[kv].at[pl.ds(start, BLOCK), columns(c)],
            dst_ref=halo.at[side, kv, :, columns(c)],
            send_sem=send_sem.at[side, kv, c],
            recv_sem=recv_sem.at[side, kv, c],
            device_id=coords(neighbour(side)),
            device_id_type=MESH,
        )

    def hand(kv, c):
        start = pl.multiple_of((rows - BLOCK) * (1 - second), BLOCK)
        return pltpu.make_async_remote_copy(
            src_ref=(k_hbm, v_hbm)[kv].at[pl.ds(start, BLOCK), columns(c)],
            dst_ref=relay.at[kv, :, columns(c)],
            send_sem=send_sem.at[second, kv, c],
            recv_sem=relay_recv.at[kv, c],
            device_id=coords(jnp.clip(via, 0, devices - 1)),
            device_id_type=MESH,
        )

    def forward(kv, c):
        return pltpu.make_async_remote_copy(
            src_ref=relay.at[kv, :, columns(c)],
            dst_ref=halo.at[target_side, kv, :, columns(c)],
            send_sem=relay_send.at[kv, c],
            recv_sem=recv_sem.at[target_side, kv, c],
            device_id=coords(jnp.clip(target, 0, devices - 1)),
            device_id_type=MESH,
        )

    def pass_on(kv, c):
        hand(kv, c).wait_recv()
        forward(kv, c).start()

    def each(lo, hi, act):
        def body(c, carry):
            for kv in range(2):
                act(kv, c)
            return carry

        lax.fori_loop(lo, hi, body, 0)

    early = min(EARLY_CHUNKS, chunks)

    def send(lo, hi):
        both = exists(first) & exists(second)

        def pair(kv, c):
            edge(first, kv, c).start()

            if not relaying:
                edge(second, kv, c).start()
                return

            @pl.when(c < handed)
            def _():
                hand(kv, c).start()

            @pl.when(c >= handed)
            def _():
                edge(second, kv, c).start()

        @pl.when(both)
        def _():
            each(lo, hi, pair)

        @pl.when(exists(first) & jnp.logical_not(both))
        def _():
            each(lo, hi, lambda kv, c: edge(first, kv, c).start())

    @pl.when(me != 1)
    def _():
        send(0, early)

    @pl.when(me == 1)
    def _():
        each(0, early, lambda kv, c: edge(first, kv, c).start())

    loads[0].wait()
    loads[1].wait()
    picks = (
        lax.broadcasted_iota(jnp.int32, (16, rows), 1) // BLOCK
        == lax.broadcasted_iota(jnp.int32, (16, rows), 0)
    ).astype(jnp.bfloat16)

    def pool(step, carry):
        for i in range(POOL_HEADS):
            h = step * POOL_HEADS + i
            cols = pl.ds(pl.multiple_of(h * HEAD_DIM, HEAD_DIM), HEAD_DIM)
            for kv, src in enumerate((k, v)):
                mean = dot(picks, src[:, cols])[:8] * (1.0 / BLOCK)
                spread = jnp.mean(mean * mean, axis=-1, keepdims=True)
                scaled = mean / jnp.sqrt(spread + 1e-06)
                for b in range(blocks):
                    own[pl.ds((kv * blocks + b) * heads + h, 1), :] = scaled[b : b + 1]
        return carry

    lax.fori_loop(0, heads // POOL_HEADS, pool, 0)
    digits = [(lane >> bit) % 2 for bit in reversed(range(bits))]
    gathered[(plane, *digits, s)] = own[...].astype(jnp.bfloat16)

    def seq_copy(o):
        mine = gathered.at[(pl.ds(plane, 1), *(pl.ds(d, 1) for d in digits), pl.ds(s, 1))]
        return pltpu.make_async_remote_copy(
            src_ref=mine,
            dst_ref=mine,
            send_sem=seq_send.at[o],
            recv_sem=seq_recv.at[o],
            device_id=(g, lax.rem(s + o, seqs)),
            device_id_type=MESH,
        )

    for o in range(1, seqs):
        seq_copy(o).start()

    if relaying:
        @pl.when(far & jnp.logical_not(odd))
        def _():
            each(0, passing, pass_on)

    @pl.when(me != 1)
    def _():
        send(early, chunks)

    @pl.when(me == 1)
    def _():
        each(early, chunks, lambda kv, c: edge(first, kv, c).start())
        each(0, chunks, lambda kv, c: edge(second, kv, c).start())

    loads[3].wait()
    loads[4].wait()
    ids = lax.broadcasted_iota(jnp.int32, (BLOCK, total_blocks), 1)
    spots = lax.broadcasted_iota(jnp.int32, (BLOCK, total_blocks), 0)
    for b in range(blocks):
        seen = spots == pos_ref[b]
        for link in range(layout_ref.shape[1]):
            seen = seen | (ids == layout_ref[b, link])
        bias[b * BLOCK : (b + 1) * BLOCK, :] = jnp.where(seen, 0.0, -jnp.inf)

    @pl.when(jnp.logical_not(has_left))
    def _():
        halo[0] = jnp.zeros(halo.shape[1:], halo.dtype)

    @pl.when(jnp.logical_not(has_right))
    def _():
        halo[1] = jnp.zeros(halo.shape[1:], halo.dtype)

    for o in range(1, seqs):
        seq_copy(o).wait()

    def line_copy(way, step):
        there = jnp.clip(plane + 1 - 2 * way, 0, planes - 1)
        part = jnp.clip(plane + (step - 1) * (2 * way - 1), 0, planes - 1)
        part = gathered.at[(pl.ds(part, 1), *(pl.ds(d, 1) for d in digits))]
        return pltpu.make_async_remote_copy(
            src_ref=part,
            dst_ref=part,
            send_sem=line_send.at[way, step],
            recv_sem=line_recv.at[way, step],
            device_id=(there * low + lane, s),
            device_id_type=MESH,
        )

    def line_sends(way, step):
        if way == 0:
            return (plane < planes - 1) & (plane - step + 1 >= 0)
        return (plane > 0) & (plane + step - 1 < planes)

    def line_gets(way, step):
        return plane - step >= 0 if way == 0 else plane + step < planes

    for step in range(1, planes):
        for way in range(2):
            @pl.when(line_sends(way, step))
            def _(way=way, step=step):
                line_copy(way, step).start()
        for way in range(2):
            @pl.when(line_gets(way, step))
            def _(way=way, step=step):
                line_copy(way, step).wait_recv()

    def bit_copy(i):
        part = gathered.at[
            (slice(None), *(slice(None) if n < i else pl.ds(d, 1) for n, d in enumerate(digits)))
        ]
        return pltpu.make_async_remote_copy(
            src_ref=part,
            dst_ref=part,
            send_sem=bit_send.at[i],
            recv_sem=bit_recv.at[i],
            device_id=(g ^ (1 << (bits - 1 - i)), s),
            device_id_type=MESH,
        )

    for i in range(bits):
        bit_copy(i).start()
        bit_copy(i).wait()

    def widen(d, carry):
        spread = blocks * heads
        at = pl.ds(pl.multiple_of(d * spread, spread), spread)
        for kv in range(2):
            spot = d // seqs
            spot = (spot // low, *((spot >> bit) % 2 for bit in reversed(range(bits))), d % seqs)
            wide[kv, at, :] = gathered[(*spot, pl.ds(kv * spread, spread))].astype(jnp.float32)
        return carry

    lax.fori_loop(0, devices, widen, 0)
    loads[2].wait()

    factor = math.log2(math.e) / math.sqrt(HEAD_DIM)
    left_bias = jnp.where(has_left, 0.0, -jnp.inf)
    right_bias = jnp.where(has_right, 0.0, -jnp.inf)

    def attend(c, carry):
        if relaying:
            @pl.when(far & odd & (c < passing))
            def _():
                for kv in range(2):
                    pass_on(kv, c)

        for side, there in ((0, has_left), (1, has_right)):
            @pl.when(there)
            def _(side=side):
                for kv in range(2):
                    edge(side, kv, c).wait_recv()

        for i in range(CHUNK_HEADS):
            h = c * CHUNK_HEADS + i
            cols = pl.ds(pl.multiple_of(h * HEAD_DIM, HEAD_DIM), HEAD_DIM)
            rows_of = pl.ds(h, total_blocks, stride=heads)
            qh, kh, vh = q[:, cols], k[:, cols], v[:, cols]
            sk = wide[0, rows_of, :].astype(jnp.bfloat16)
            sv = wide[1, rows_of, :].astype(jnp.bfloat16)
            kl, vl = halo[0, 0, :, cols], halo[0, 1, :, cols]
            kr, vr = halo[1, 0, :, cols], halo[1, 1, :, cols]
            s_own = dot_t(qh, kh)
            if blocks > 2:
                gap = (
                    lax.broadcasted_iota(jnp.int32, (rows, rows), 0) // BLOCK
                    - lax.broadcasted_iota(jnp.int32, (rows, rows), 1) // BLOCK
                )
                s_own = jnp.where(jnp.abs(gap) <= 1, s_own, -jnp.inf)
            s_left = dot_t(qh[:BLOCK], kl) + left_bias
            s_right = dot_t(qh[rows - BLOCK :], kr) + right_bias
            s_sum = dot_t(qh, sk) + bias[...]
            middle = [jnp.full((rows - 2 * BLOCK, BLOCK), -jnp.inf)] if blocks > 2 else []
            s_halo = jnp.concatenate([s_left, *middle, s_right], axis=0)
            peak = jnp.maximum(
                jnp.max(s_sum, axis=-1, keepdims=True),
                jnp.maximum(
                    jnp.max(s_own, axis=-1, keepdims=True),
                    jnp.max(s_halo, axis=-1, keepdims=True),
                ),
            )
            w_own = jnp.exp2((s_own - peak) * factor)
            w_halo = jnp.exp2((s_halo - peak) * factor)
            w_sum = jnp.exp2((s_sum - peak) * factor)
            total = (
                jnp.sum(w_own, axis=-1, keepdims=True)
                + jnp.sum(w_halo, axis=-1, keepdims=True)
                + jnp.sum(w_sum, axis=-1, keepdims=True)
            )
            r_halo = w_halo.astype(jnp.bfloat16)
            acc = dot(w_own.astype(jnp.bfloat16), vh) + dot(w_sum.astype(jnp.bfloat16), sv)
            middle = [jnp.zeros((rows - 2 * BLOCK, HEAD_DIM), jnp.float32)] if blocks > 2 else []
            acc = acc + jnp.concatenate(
                [dot(r_halo[:BLOCK], vl), *middle, dot(r_halo[rows - BLOCK :], vr)], axis=0
            )
            out[:, cols] = (acc / total).astype(jnp.bfloat16)
        return carry

    lax.fori_loop(0, chunks, attend, 0)

    for side in range(2):
        @pl.when(exists(side))
        def _(side=side):
            each(0, chunks, lambda kv, c: edge(side, kv, c).wait_send())

    if relaying:
        @pl.when(far)
        def _():
            each(0, passing, lambda kv, c: forward(kv, c).wait_send())

    for step in range(1, planes):
        for way in range(2):
            @pl.when(line_sends(way, step))
            def _(way=way, step=step):
                line_copy(way, step).wait_send()


def gather_shape(groups):
    bits = min(groups.bit_length() - 1, PLANE_BITS)
    return bits, groups >> bits


def relays(groups, seqs):
    return seqs == 2 and groups >= 8


def solution(mesh):
    groups, seqs = mesh.shape["grp"], mesh.shape["seq"]
    assert groups & (groups - 1) == 0

    def shards(queries, keys, values, global_pos, layout):
        rows, width = queries.shape
        blocks, heads = rows // BLOCK, width // HEAD_DIM
        devices = groups * seqs
        chunks = heads // CHUNK_HEADS
        bits, planes = gather_shape(groups)
        summaries = devices * blocks * width
        limit = 2 * (4 * rows + 6 * BLOCK) * width + 12 * summaries + (8 << 20)
        operands = [
            pltpu.with_memory_space_constraint(a, pltpu.HBM)
            for a in (global_pos, layout, queries, keys, values)
        ]
        return pl.pallas_call(
            functools.partial(kernel, groups, seqs),
            out_shape=pltpu.VMEM((rows, width), jnp.bfloat16),
            in_specs=[pl.BlockSpec(memory_space=pltpu.HBM)] * 5,
            out_specs=pl.BlockSpec(memory_space=pltpu.VMEM),
            scratch_shapes=[
                pltpu.SMEM(global_pos.shape, jnp.int32),
                pltpu.SMEM(layout.shape, jnp.int32),
                pltpu.VMEM((rows, width), jnp.bfloat16),
                pltpu.VMEM((rows, width), jnp.bfloat16),
                pltpu.VMEM((rows, width), jnp.bfloat16),
                pltpu.VMEM((2, 2, BLOCK, width), jnp.bfloat16),
                pltpu.VMEM((2, BLOCK, width), jnp.bfloat16),
                pltpu.VMEM((planes, *(2,) * bits, seqs, 2 * blocks * heads, HEAD_DIM), jnp.bfloat16),
                pltpu.VMEM((2 * blocks * heads, HEAD_DIM), jnp.float32),
                pltpu.VMEM((2, devices * blocks * heads, HEAD_DIM), jnp.float32),
                pltpu.VMEM((rows, devices * blocks), jnp.float32),
                pltpu.SemaphoreType.DMA((5,)),
                pltpu.SemaphoreType.DMA((2, 2, chunks)),
                pltpu.SemaphoreType.DMA((2, 2, chunks)),
                pltpu.SemaphoreType.DMA((2, chunks)),
                pltpu.SemaphoreType.DMA((2, chunks)),
                pltpu.SemaphoreType.DMA((seqs,)),
                pltpu.SemaphoreType.DMA((seqs,)),
                pltpu.SemaphoreType.DMA((2, planes)),
                pltpu.SemaphoreType.DMA((2, planes)),
                pltpu.SemaphoreType.DMA((max(bits, 1),)),
                pltpu.SemaphoreType.DMA((max(bits, 1),)),
            ],
            compiler_params=pltpu.CompilerParams(
                collective_id=0, has_side_effects=True, vmem_limit_bytes=limit
            ),
        )(*operands)

    both = ("grp", "seq")
    in_specs = (P(both, None), P(both, None), P(both, None), P(both), P(both, None))
    return jax.shard_map(
        shards, mesh=mesh, in_specs=in_specs, out_specs=P(both, None), check_vma=False
    )
```

```python
import functools
import math

import jax
import jax.numpy as jnp
from jax import lax
from jax.experimental import pallas as pl
from jax.experimental.pallas import tpu as pltpu
from jax.sharding import PartitionSpec as P

HEAD_DIM = 128
BLOCK = 128
STEP_HEADS = 2
UNIT_HEADS = 4
TAPER = (2, 1, 1)
EARLY_UNITS = 1
LEAD_UNITS = 1
PLANE_BITS = 2
POOL_HEADS = 8
MESH = pl.DeviceIdType.MESH


def dot_t(a, b):
    return lax.dot_general(a, b, (((1,), (1,)), ((), ())), preferred_element_type=jnp.float32)


def dot(a, b):
    return jnp.dot(a, b, preferred_element_type=jnp.float32)


def kernel(
    groups, seqs, pos_hbm, layout_hbm, q_hbm, k_hbm, v_hbm, out,
    pos_ref, layout_ref, q, kv_own, halo, relay, gathered, own, wide, bias,
    load_sem, send_sem, recv_sem, relay_recv, relay_send, seq_send, seq_recv,
    line_send, line_recv, bit_send, bit_recv,
):
    rows, width = q.shape
    k, v = kv_own.at[0], kv_own.at[1]
    heads = width // HEAD_DIM
    blocks = rows // BLOCK
    devices = groups * seqs
    total_blocks = devices * blocks
    bits, planes = gather_shape(groups)
    low = 1 << bits
    relaying = relays(groups, seqs)

    g, s = lax.axis_index("grp"), lax.axis_index("seq")
    me = g * seqs + s
    has_left, has_right = me > 0, me < devices - 1
    plane, lane = g // low, g % low

    def coords(position):
        return (position // seqs, position % seqs)

    first = s % 2
    second = 1 - first

    def exists(side):
        return jnp.where(side == 0, has_right, has_left)

    def neighbour(side):
        return jnp.clip(me + 1 - 2 * side, 0, devices - 1)

    pairs = groups // 2
    step_pair = 2 * seqs
    far = (g % 2 == s) if relaying else False
    rank = jnp.where(s == 0, g // 2, pairs - 1 - g // 2)
    odd = rank % 2 == 1
    across = me + (step_pair - 1) * (1 - 2 * s)
    behind, ahead = me + step_pair * (1 - 2 * s), me - step_pair * (1 - 2 * s)
    handed = jnp.where(far, heads * jnp.where(odd, 1, rank) // (pairs * UNIT_HEADS), 0) if relaying else 0
    via = jnp.where(odd, ahead, across)
    passing = heads * jnp.where(odd, pairs - 1 - rank, 1) // (pairs * UNIT_HEADS)
    target = jnp.where(odd, behind, across)
    target_side = jnp.where(odd, first, second)
    apart = (s == 1) & (g < 2) if relaying else False
    lead, lead_relay = apart & (g == 0), apart & (g == 1)
    hand_side = jnp.where(lead, first, second)
    if relaying:
        handed = jnp.where(lead, LEAD_UNITS, handed)
        via = jnp.where(lead, me + seqs, via)
        passing = jnp.where(lead_relay, LEAD_UNITS, passing)
        target = jnp.where(lead_relay, across, target)
    at_once = jnp.logical_not(odd) | lead_relay

    units, taper = edge_units(heads)
    early = min(EARLY_UNITS, units)
    split = early * UNIT_HEADS * HEAD_DIM
    ahead_cols, rest_cols = pl.ds(0, split), pl.ds(split, width - split)
    moves = [(x.at[:, part], y.at[:, part]) for part in (ahead_cols, rest_cols) for x, y in ((k_hbm, k), (v_hbm, v))]
    moves += [(q_hbm, q), (pos_hbm, pos_ref), (layout_hbm, layout_ref)]
    loads = [pltpu.make_async_copy(x, y, load_sem.at[i]) for i, (x, y) in enumerate(moves)]
    for load in loads[:2]:
        load.start()
    barrier = pltpu.get_barrier_semaphore()

    peers = [(exists(side), neighbour(side)) for side in range(2)]
    peers += [(True, g * seqs + lax.rem(s + o, seqs)) for o in range(1, seqs)]
    peers += [(True, (g ^ (1 << bit)) * seqs + s) for bit in range(bits)]
    if planes > 1:
        peers += [
            (plane > 0, jnp.maximum(me - low * seqs, 0)),
            (plane < planes - 1, jnp.minimum(me + low * seqs, devices - 1)),
        ]
    if relaying:
        peers += [(far, across), (far & (rank > 0), ahead), (far & (rank < pairs - 1), behind)]
    expected = 0
    for there, peer in peers:
        if there is True:
            pl.semaphore_signal(barrier, inc=1, device_id=coords(peer), device_id_type=MESH)
            expected = expected + 1
        else:
            @pl.when(there)
            def _(peer=peer):
                pl.semaphore_signal(barrier, inc=1, device_id=coords(peer), device_id_type=MESH)
            expected = expected + there.astype(jnp.int32)
    for load in loads[2:]:
        load.start()
    pl.semaphore_wait(barrier, expected)

    def columns(h):
        return pl.ds(pl.multiple_of(h * HEAD_DIM, HEAD_DIM), HEAD_DIM)

    def span(u):
        if isinstance(u, int) and u >= units:
            lo, n = taper[u - units]
            return pl.ds(lo * HEAD_DIM, n * HEAD_DIM)
        return pl.ds(pl.multiple_of(u * UNIT_HEADS * HEAD_DIM, UNIT_HEADS * HEAD_DIM), UNIT_HEADS * HEAD_DIM)

    def edge(side, u):
        start = pl.multiple_of((rows - BLOCK) * (1 - side), BLOCK)
        return pltpu.make_async_remote_copy(
            src_ref=kv_own.at[:, pl.ds(start, BLOCK), span(u)],
            dst_ref=halo.at[side, :, :, span(u)],
            send_sem=send_sem.at[side, u],
            recv_sem=recv_sem.at[side, u],
            device_id=coords(neighbour(side)),
            device_id_type=MESH,
        )

    def hand(u):
        start = pl.multiple_of((rows - BLOCK) * (1 - hand_side), BLOCK)
        return pltpu.make_async_remote_copy(
            src_ref=kv_own.at[:, pl.ds(start, BLOCK), span(u)],
            dst_ref=relay.at[:, :, span(u)],
            send_sem=send_sem.at[hand_side, u],
            recv_sem=relay_recv.at[u],
            device_id=coords(jnp.clip(via, 0, devices - 1)),
            device_id_type=MESH,
        )

    def forward(u):
        return pltpu.make_async_remote_copy(
            src_ref=relay.at[:, :, span(u)],
            dst_ref=halo.at[target_side, :, :, span(u)],
            send_sem=relay_send.at[u],
            recv_sem=recv_sem.at[target_side, u],
            device_id=coords(jnp.clip(target, 0, devices - 1)),
            device_id_type=MESH,
        )

    def pass_on(u):
        hand(u).wait_recv()
        forward(u).start()

    def each(lo, hi, act):
        def body(u, carry):
            act(u)
            return carry

        lax.fori_loop(lo, hi, body, 0)

    def every(lo, act):
        each(lo, units, act)
        for i in range(len(taper)):
            act(units + i)

    def send(sides):
        def act(u):
            for side in sides:
                if not relaying or (isinstance(u, int) and u >= units):
                    edge(side, u).start()
                    continue
                stop = (u < handed) & (side == hand_side)

                @pl.when(stop)
                def _():
                    hand(u).start()

                @pl.when(jnp.logical_not(stop))
                def _(side=side):
                    edge(side, u).start()

        return act

    both = exists(first) & exists(second) & jnp.logical_not(apart)

    loads[0].wait()
    loads[1].wait()

    @pl.when(both)
    def _():
        each(0, early, send((first, second)))

    @pl.when(exists(first) & jnp.logical_not(both))
    def _():
        each(0, early, send((first,)))

    loads[2].wait()
    loads[3].wait()
    picks = (
        lax.broadcasted_iota(jnp.int32, (16, rows), 1) // BLOCK
        == lax.broadcasted_iota(jnp.int32, (16, rows), 0)
    ).astype(jnp.bfloat16)

    def pool(step, carry):
        for i in range(POOL_HEADS):
            h = step * POOL_HEADS + i
            cols = columns(h)
            for kv, src in enumerate((k, v)):
                mean = dot(picks, src[:, cols])[:8] * (1.0 / BLOCK)
                spread = jnp.mean(mean * mean, axis=-1, keepdims=True)
                scaled = mean / jnp.sqrt(spread + 1e-06)
                for b in range(blocks):
                    own[pl.ds((kv * blocks + b) * heads + h, 1), :] = scaled[b : b + 1]
        return carry

    lax.fori_loop(0, heads // POOL_HEADS, pool, 0)
    digits = [(lane >> bit) % 2 for bit in reversed(range(bits))]
    gathered[(plane, *digits, s)] = own[...].astype(jnp.bfloat16)

    def seq_copy(o):
        mine = gathered.at[(pl.ds(plane, 1), *(pl.ds(d, 1) for d in digits), pl.ds(s, 1))]
        return pltpu.make_async_remote_copy(
            src_ref=mine,
            dst_ref=mine,
            send_sem=seq_send.at[o],
            recv_sem=seq_recv.at[o],
            device_id=(g, lax.rem(s + o, seqs)),
            device_id_type=MESH,
        )

    for o in range(1, seqs):
        seq_copy(o).start()

    if relaying:
        @pl.when(far & at_once)
        def _():
            each(0, passing, pass_on)

    @pl.when(both)
    def _():
        every(early, send((first, second)))

    @pl.when(exists(first) & jnp.logical_not(both))
    def _():
        every(early, send((first,)))

    @pl.when(exists(second) & apart)
    def _():
        every(0, send((second,)))

    loads[5].wait()
    loads[6].wait()
    ids = lax.broadcasted_iota(jnp.int32, (BLOCK, total_blocks), 1)
    spots = lax.broadcasted_iota(jnp.int32, (BLOCK, total_blocks), 0)
    for b in range(blocks):
        seen = spots == pos_ref[b]
        for link in range(layout_ref.shape[1]):
            seen = seen | (ids == layout_ref[b, link])
        bias[b * BLOCK : (b + 1) * BLOCK, :] = jnp.where(seen, 0.0, -jnp.inf)

    @pl.when(jnp.logical_not(has_left))
    def _():
        halo[0] = jnp.zeros(halo.shape[1:], halo.dtype)

    @pl.when(jnp.logical_not(has_right))
    def _():
        halo[1] = jnp.zeros(halo.shape[1:], halo.dtype)

    for o in range(1, seqs):
        seq_copy(o).wait()

    def line_copy(way, step):
        there = jnp.clip(plane + 1 - 2 * way, 0, planes - 1)
        part = jnp.clip(plane + (step - 1) * (2 * way - 1), 0, planes - 1)
        part = gathered.at[(pl.ds(part, 1), *(pl.ds(d, 1) for d in digits))]
        return pltpu.make_async_remote_copy(
            src_ref=part,
            dst_ref=part,
            send_sem=line_send.at[way, step],
            recv_sem=line_recv.at[way, step],
            device_id=(there * low + lane, s),
            device_id_type=MESH,
        )

    def line_sends(way, step):
        if way == 0:
            return (plane < planes - 1) & (plane - step + 1 >= 0)
        return (plane > 0) & (plane + step - 1 < planes)

    def line_gets(way, step):
        return plane - step >= 0 if way == 0 else plane + step < planes

    for step in range(1, planes):
        for way in range(2):
            @pl.when(line_sends(way, step))
            def _(way=way, step=step):
                line_copy(way, step).start()
        for way in range(2):
            @pl.when(line_gets(way, step))
            def _(way=way, step=step):
                line_copy(way, step).wait_recv()

    def bit_copy(i):
        part = gathered.at[
            (slice(None), *(slice(None) if n < i else pl.ds(d, 1) for n, d in enumerate(digits)))
        ]
        return pltpu.make_async_remote_copy(
            src_ref=part,
            dst_ref=part,
            send_sem=bit_send.at[i],
            recv_sem=bit_recv.at[i],
            device_id=(g ^ (1 << (bits - 1 - i)), s),
            device_id_type=MESH,
        )

    for i in range(bits):
        bit_copy(i).start()
        bit_copy(i).wait()

    def widen(d, carry):
        spread = blocks * heads
        at = pl.ds(pl.multiple_of(d * spread, spread), spread)
        for kv in range(2):
            spot = d // seqs
            spot = (spot // low, *((spot >> bit) % 2 for bit in reversed(range(bits))), d % seqs)
            wide[kv, at, :] = gathered[(*spot, pl.ds(kv * spread, spread))].astype(jnp.float32)
        return carry

    lax.fori_loop(0, devices, widen, 0)
    loads[4].wait()

    factor = math.log2(math.e) / math.sqrt(HEAD_DIM)
    left_bias = jnp.where(has_left, 0.0, -jnp.inf)
    right_bias = jnp.where(has_right, 0.0, -jnp.inf)

    def attend_head(h, ready):
        cols = columns(h)
        rows_of = pl.ds(h, total_blocks, stride=heads)
        qh, kh, vh = q[:, cols], k[:, cols], v[:, cols]
        sk = wide[0, rows_of, :].astype(jnp.bfloat16)
        sv = wide[1, rows_of, :].astype(jnp.bfloat16)
        s_own = dot_t(qh, kh)
        if blocks > 2:
            gap = (
                lax.broadcasted_iota(jnp.int32, (rows, rows), 0) // BLOCK
                - lax.broadcasted_iota(jnp.int32, (rows, rows), 1) // BLOCK
            )
            s_own = jnp.where(jnp.abs(gap) <= 1, s_own, -jnp.inf)
        s_sum = dot_t(qh, sk) + bias[...]
        ready()
        s_left = dot_t(qh[:BLOCK], halo[0, 0, :, cols]) + left_bias
        s_right = dot_t(qh[rows - BLOCK :], halo[1, 0, :, cols]) + right_bias
        middle = [jnp.full((rows - 2 * BLOCK, BLOCK), -jnp.inf)] if blocks > 2 else []
        s_halo = jnp.concatenate([s_left, *middle, s_right], axis=0)
        peak = jnp.maximum(
            jnp.max(s_sum, axis=-1, keepdims=True),
            jnp.maximum(
                jnp.max(s_own, axis=-1, keepdims=True),
                jnp.max(s_halo, axis=-1, keepdims=True),
            ),
        )
        w_own = jnp.exp2((s_own - peak) * factor)
        w_halo = jnp.exp2((s_halo - peak) * factor)
        w_sum = jnp.exp2((s_sum - peak) * factor)
        total = (
            jnp.sum(w_own, axis=-1, keepdims=True)
            + jnp.sum(w_halo, axis=-1, keepdims=True)
            + jnp.sum(w_sum, axis=-1, keepdims=True)
        )
        r_halo = w_halo.astype(jnp.bfloat16)
        acc = dot(w_own.astype(jnp.bfloat16), vh) + dot(w_sum.astype(jnp.bfloat16), sv)
        vl, vr = halo[0, 1, :, cols], halo[1, 1, :, cols]
        middle = [jnp.zeros((rows - 2 * BLOCK, HEAD_DIM), jnp.float32)] if blocks > 2 else []
        acc = acc + jnp.concatenate(
            [dot(r_halo[:BLOCK], vl), *middle, dot(r_halo[rows - BLOCK :], vr)], axis=0
        )
        out[:, cols] = (acc / total).astype(jnp.bfloat16)

    def arrived(u):
        for side, there in ((0, has_left), (1, has_right)):
            @pl.when(there)
            def _(side=side):
                edge(side, u).wait_recv()

    steps = UNIT_HEADS // STEP_HEADS

    def attend(step, carry):
        u = step // steps

        @pl.when(step % steps == 0)
        def _():
            if relaying:
                @pl.when(far & jnp.logical_not(at_once) & (u < passing))
                def _():
                    pass_on(u)

            arrived(u)

        for i in range(STEP_HEADS):
            attend_head(step * STEP_HEADS + i, lambda: None)
        return carry

    lax.fori_loop(0, units * steps, attend, 0)

    def sent(lo, hi):
        for side in range(2):
            @pl.when(exists(side))
            def _(side=side):
                each(lo, hi, lambda u: edge(side, u).wait_send())

    for i, (lo, n) in enumerate(taper):
        if n > 1:
            arrived(units + i)
            for h in range(lo, lo + n):
                attend_head(h, lambda: None)
            continue
        if i + 1 == len(taper):
            sent(0, units)
            if relaying:
                @pl.when(far)
                def _():
                    each(0, passing, lambda u: forward(u).wait_send())

            for step in range(1, planes):
                for way in range(2):
                    @pl.when(line_sends(way, step))
                    def _(way=way, step=step):
                        line_copy(way, step).wait_send()

        attend_head(lo, lambda i=i: arrived(units + i))

    for side in range(2):
        @pl.when(exists(side))
        def _(side=side):
            for i in range(len(taper)):
                edge(side, units + i).wait_send()


def edge_units(heads):
    units = (heads - sum(TAPER)) // UNIT_HEADS
    lo, taper = units * UNIT_HEADS, []
    for n in (heads - lo - sum(TAPER), *TAPER):
        if n:
            taper.append((lo, n))
            lo += n
    return units, taper


def gather_shape(groups):
    bits = min(groups.bit_length() - 1, PLANE_BITS)
    return bits, groups >> bits


def relays(groups, seqs):
    return seqs == 2 and groups >= 8


def solution(mesh):
    groups, seqs = mesh.shape["grp"], mesh.shape["seq"]
    assert groups & (groups - 1) == 0

    def shards(queries, keys, values, global_pos, layout):
        rows, width = queries.shape
        blocks, heads = rows // BLOCK, width // HEAD_DIM
        devices = groups * seqs
        units, taper = edge_units(heads)
        units += len(taper)
        bits, planes = gather_shape(groups)
        summaries = devices * blocks * width
        limit = 2 * (4 * rows + 6 * BLOCK) * width + 12 * summaries + (8 << 20)
        operands = [
            pltpu.with_memory_space_constraint(a, pltpu.HBM)
            for a in (global_pos, layout, queries, keys, values)
        ]
        return pl.pallas_call(
            functools.partial(kernel, groups, seqs),
            out_shape=pltpu.VMEM((rows, width), jnp.bfloat16),
            in_specs=[pl.BlockSpec(memory_space=pltpu.HBM)] * 5,
            out_specs=pl.BlockSpec(memory_space=pltpu.VMEM),
            scratch_shapes=[
                pltpu.SMEM(global_pos.shape, jnp.int32),
                pltpu.SMEM(layout.shape, jnp.int32),
                pltpu.VMEM((rows, width), jnp.bfloat16),
                pltpu.VMEM((2, rows, width), jnp.bfloat16),
                pltpu.VMEM((2, 2, BLOCK, width), jnp.bfloat16),
                pltpu.VMEM((2, BLOCK, width), jnp.bfloat16),
                pltpu.VMEM((planes, *(2,) * bits, seqs, 2 * blocks * heads, HEAD_DIM), jnp.bfloat16),
                pltpu.VMEM((2 * blocks * heads, HEAD_DIM), jnp.float32),
                pltpu.VMEM((2, devices * blocks * heads, HEAD_DIM), jnp.float32),
                pltpu.VMEM((rows, devices * blocks), jnp.float32),
                pltpu.SemaphoreType.DMA((7,)),
                pltpu.SemaphoreType.DMA((2, units)),
                pltpu.SemaphoreType.DMA((2, units)),
                pltpu.SemaphoreType.DMA((units,)),
                pltpu.SemaphoreType.DMA((units,)),
                pltpu.SemaphoreType.DMA((seqs,)),
                pltpu.SemaphoreType.DMA((seqs,)),
                pltpu.SemaphoreType.DMA((2, planes)),
                pltpu.SemaphoreType.DMA((2, planes)),
                pltpu.SemaphoreType.DMA((max(bits, 1),)),
                pltpu.SemaphoreType.DMA((max(bits, 1),)),
            ],
            compiler_params=pltpu.CompilerParams(
                collective_id=0, has_side_effects=True, vmem_limit_bytes=limit
            ),
        )(*operands)

    both = ("grp", "seq")
    in_specs = (P(both, None), P(both, None), P(both, None), P(both), P(both, None))
    return jax.shard_map(
        shards, mesh=mesh, in_specs=in_specs, out_specs=P(both, None), check_vma=False
    )
```

```python
import functools
import math

import jax
import jax.numpy as jnp
from jax import lax
from jax.experimental import pallas as pl
from jax.experimental.pallas import tpu as pltpu
from jax.sharding import PartitionSpec as P

HEAD_DIM = 128
BLOCK = 128
STEP_HEADS = 2
UNIT_HEADS = 4
TAPER = (2, 1, 1)
EARLY_UNITS = 1
LEAD_UNITS = 1
LEAD_TAPER = 1
SWAP = True
PLANE_BITS = 2
POOL_HEADS = 8
MESH = pl.DeviceIdType.MESH


def dot_t(a, b):
    return lax.dot_general(a, b, (((1,), (1,)), ((), ())), preferred_element_type=jnp.float32)


def dot(a, b):
    return jnp.dot(a, b, preferred_element_type=jnp.float32)


def kernel(
    groups, seqs, pos_hbm, layout_hbm, q_hbm, k_hbm, v_hbm, out,
    pos_ref, layout_ref, q, kv_own, halo, relay, gathered, own, wide, bias,
    load_sem, send_sem, recv_sem, relay_recv, relay_send, seq_send, seq_recv,
    line_send, line_recv, bit_send, bit_recv,
):
    rows, width = q.shape
    k, v = kv_own.at[0], kv_own.at[1]
    heads = width // HEAD_DIM
    blocks = rows // BLOCK
    devices = groups * seqs
    total_blocks = devices * blocks
    bits, planes = gather_shape(groups)
    low = 1 << bits
    relaying = relays(groups, seqs)

    g, s = lax.axis_index("grp"), lax.axis_index("seq")
    me = g * seqs + s
    has_left, has_right = me > 0, me < devices - 1
    plane, lane = g // low, g % low

    def coords(position):
        return (position // seqs, position % seqs)

    first = s % 2
    second = 1 - first

    def exists(side):
        return jnp.where(side == 0, has_right, has_left)

    def neighbour(side):
        return jnp.clip(me + 1 - 2 * side, 0, devices - 1)

    pairs = groups // 2
    step_pair = 2 * seqs
    far = (g % 2 == s) if relaying else False
    rank = jnp.where(s == 0, g // 2, pairs - 1 - g // 2)
    odd = rank % 2 == 1
    across = me + (step_pair - 1) * (1 - 2 * s)
    behind, ahead = me + step_pair * (1 - 2 * s), me - step_pair * (1 - 2 * s)
    handed = jnp.where(far, heads * jnp.where(odd, 1, rank) // (pairs * UNIT_HEADS), 0) if relaying else 0
    via = jnp.where(odd, ahead, across)
    passing = heads * jnp.where(odd, pairs - 1 - rank, 1) // (pairs * UNIT_HEADS)
    target = jnp.where(odd, behind, across)
    target_side = jnp.where(odd, first, second)
    apart = (s == 1) & (g < 2) if relaying else False
    lead, lead_relay = apart & (g == 0), apart & (g == 1)
    hand_side = jnp.where(lead, first, second)
    if relaying:
        handed = jnp.where(lead, LEAD_UNITS, handed)
        via = jnp.where(lead, me + seqs, via)
        passing = jnp.where(lead_relay, LEAD_UNITS, passing)
        target = jnp.where(lead_relay, across, target)
    at_once = jnp.logical_not(odd) | lead_relay

    units, taper = edge_units(heads)
    early = min(EARLY_UNITS, units)
    split = early * UNIT_HEADS * HEAD_DIM
    ahead_cols, rest_cols = pl.ds(0, split), pl.ds(split, width - split)
    moves = [(x.at[:, part], y.at[:, part]) for part in (ahead_cols, rest_cols) for x, y in ((k_hbm, k), (v_hbm, v))]
    moves += [(q_hbm, q), (pos_hbm, pos_ref), (layout_hbm, layout_ref)]
    loads = [pltpu.make_async_copy(x, y, load_sem.at[i]) for i, (x, y) in enumerate(moves)]
    barrier = pltpu.get_barrier_semaphore()

    peers = [(True, g * seqs + lax.rem(s + o, seqs)) for o in range(1, seqs)]
    if seqs == 2:
        peers += [(exists(second), neighbour(second))]
    else:
        peers += [(exists(side), neighbour(side)) for side in range(2)]
    peers += [(True, (g ^ (1 << bit)) * seqs + s) for bit in range(bits)]
    if planes > 1:
        peers += [
            (plane > 0, jnp.maximum(me - low * seqs, 0)),
            (plane < planes - 1, jnp.minimum(me + low * seqs, devices - 1)),
        ]
    if relaying:
        peers += [(far, across), (far & (rank > 0), ahead), (far & (rank < pairs - 1), behind)]
    expected = 0
    for there, peer in peers:
        if there is True:
            pl.semaphore_signal(barrier, inc=1, device_id=coords(peer), device_id_type=MESH)
            expected = expected + 1
        else:
            @pl.when(there)
            def _(peer=peer):
                pl.semaphore_signal(barrier, inc=1, device_id=coords(peer), device_id_type=MESH)
            expected = expected + there.astype(jnp.int32)
    for load in loads:
        load.start()
    pl.semaphore_wait(barrier, expected)

    def columns(h):
        return pl.ds(pl.multiple_of(h * HEAD_DIM, HEAD_DIM), HEAD_DIM)

    def span(u):
        if isinstance(u, int) and u >= units:
            lo, n = taper[u - units]
            return pl.ds(lo * HEAD_DIM, n * HEAD_DIM)
        return pl.ds(pl.multiple_of(u * UNIT_HEADS * HEAD_DIM, UNIT_HEADS * HEAD_DIM), UNIT_HEADS * HEAD_DIM)

    def edge(side, u):
        start = pl.multiple_of((rows - BLOCK) * (1 - side), BLOCK)
        return pltpu.make_async_remote_copy(
            src_ref=kv_own.at[:, pl.ds(start, BLOCK), span(u)],
            dst_ref=halo.at[side, :, :, span(u)],
            send_sem=send_sem.at[side, u],
            recv_sem=recv_sem.at[side, u],
            device_id=coords(neighbour(side)),
            device_id_type=MESH,
        )

    def hand(u):
        start = pl.multiple_of((rows - BLOCK) * (1 - hand_side), BLOCK)
        return pltpu.make_async_remote_copy(
            src_ref=kv_own.at[:, pl.ds(start, BLOCK), span(u)],
            dst_ref=relay.at[:, :, span(u)],
            send_sem=send_sem.at[hand_side, u],
            recv_sem=relay_recv.at[u],
            device_id=coords(jnp.clip(via, 0, devices - 1)),
            device_id_type=MESH,
        )

    def forward(u):
        return pltpu.make_async_remote_copy(
            src_ref=relay.at[:, :, span(u)],
            dst_ref=halo.at[target_side, :, :, span(u)],
            send_sem=relay_send.at[u],
            recv_sem=recv_sem.at[target_side, u],
            device_id=coords(jnp.clip(target, 0, devices - 1)),
            device_id_type=MESH,
        )

    def pass_on(u):
        hand(u).wait_recv()
        forward(u).start()

    def each(lo, hi, act):
        def body(u, carry):
            act(u)
            return carry

        lax.fori_loop(lo, hi, body, 0)

    def every(lo, act):
        each(lo, units, act)
        for i in range(len(taper)):
            act(units + i)

    def send(sides):
        def act(u):
            for side in sides:
                if not relaying or (isinstance(u, int) and u >= units and u != units + LEAD_TAPER):
                    edge(side, u).start()
                    continue
                stop = (lead if isinstance(u, int) and u >= units else u < handed) & (side == hand_side)

                @pl.when(stop)
                def _():
                    hand(u).start()

                @pl.when(jnp.logical_not(stop))
                def _(side=side):
                    edge(side, u).start()

        return act

    ahead_side = jnp.where((s == 1) & (g % 2 == 0), second, first) if SWAP else first
    both = exists(first) & exists(second) & jnp.logical_not(apart)

    loads[0].wait()
    loads[1].wait()

    @pl.when(both)
    def _():
        each(0, early, send((ahead_side, 1 - ahead_side)))

    @pl.when(exists(first) & jnp.logical_not(both))
    def _():
        each(0, early, send((first,)))

    loads[2].wait()
    loads[3].wait()
    picks = (
        lax.broadcasted_iota(jnp.int32, (16, rows), 1) // BLOCK
        == lax.broadcasted_iota(jnp.int32, (16, rows), 0)
    ).astype(jnp.bfloat16)

    def pool(step, carry):
        for i in range(POOL_HEADS):
            h = step * POOL_HEADS + i
            cols = columns(h)
            for kv, src in enumerate((k, v)):
                mean = dot(picks, src[:, cols])[:8] * (1.0 / BLOCK)
                spread = jnp.mean(mean * mean, axis=-1, keepdims=True)
                scaled = mean / jnp.sqrt(spread + 1e-06)
                for b in range(blocks):
                    own[pl.ds((kv * blocks + b) * heads + h, 1), :] = scaled[b : b + 1]
        return carry

    lax.fori_loop(0, heads // POOL_HEADS, pool, 0)
    digits = [(lane >> bit) % 2 for bit in reversed(range(bits))]
    gathered[(plane, *digits, s)] = own[...].astype(jnp.bfloat16)

    def seq_copy(o):
        mine = gathered.at[(pl.ds(plane, 1), *(pl.ds(d, 1) for d in digits), pl.ds(s, 1))]
        return pltpu.make_async_remote_copy(
            src_ref=mine,
            dst_ref=mine,
            send_sem=seq_send.at[o],
            recv_sem=seq_recv.at[o],
            device_id=(g, lax.rem(s + o, seqs)),
            device_id_type=MESH,
        )

    for o in range(1, seqs):
        seq_copy(o).start()

    if relaying:
        @pl.when(far & at_once)
        def _():
            each(0, passing, pass_on)

        @pl.when(lead_relay)
        def _():
            pass_on(units + LEAD_TAPER)

    @pl.when(both)
    def _():
        every(early, send((ahead_side, 1 - ahead_side)))

    @pl.when(exists(first) & jnp.logical_not(both))
    def _():
        every(early, send((first,)))

    @pl.when(exists(second) & apart)
    def _():
        every(0, send((second,)))

    loads[5].wait()
    loads[6].wait()
    ids = lax.broadcasted_iota(jnp.int32, (BLOCK, total_blocks), 1)
    spots = lax.broadcasted_iota(jnp.int32, (BLOCK, total_blocks), 0)
    for b in range(blocks):
        seen = spots == pos_ref[b]
        for link in range(layout_ref.shape[1]):
            seen = seen | (ids == layout_ref[b, link])
        bias[b * BLOCK : (b + 1) * BLOCK, :] = jnp.where(seen, 0.0, -jnp.inf)

    @pl.when(jnp.logical_not(has_left))
    def _():
        halo[0] = jnp.zeros(halo.shape[1:], halo.dtype)

    @pl.when(jnp.logical_not(has_right))
    def _():
        halo[1] = jnp.zeros(halo.shape[1:], halo.dtype)

    for o in range(1, seqs):
        seq_copy(o).wait()

    def line_copy(way, step):
        there = jnp.clip(plane + 1 - 2 * way, 0, planes - 1)
        part = jnp.clip(plane + (step - 1) * (2 * way - 1), 0, planes - 1)
        part = gathered.at[(pl.ds(part, 1), *(pl.ds(d, 1) for d in digits))]
        return pltpu.make_async_remote_copy(
            src_ref=part,
            dst_ref=part,
            send_sem=line_send.at[way, step],
            recv_sem=line_recv.at[way, step],
            device_id=(there * low + lane, s),
            device_id_type=MESH,
        )

    def line_sends(way, step):
        if way == 0:
            return (plane < planes - 1) & (plane - step + 1 >= 0)
        return (plane > 0) & (plane + step - 1 < planes)

    def line_gets(way, step):
        return plane - step >= 0 if way == 0 else plane + step < planes

    for step in range(1, planes):
        for way in range(2):
            @pl.when(line_sends(way, step))
            def _(way=way, step=step):
                line_copy(way, step).start()
        for way in range(2):
            @pl.when(line_gets(way, step))
            def _(way=way, step=step):
                line_copy(way, step).wait_recv()

    def bit_copy(i):
        part = gathered.at[
            (slice(None), *(slice(None) if n < i else pl.ds(d, 1) for n, d in enumerate(digits)))
        ]
        return pltpu.make_async_remote_copy(
            src_ref=part,
            dst_ref=part,
            send_sem=bit_send.at[i],
            recv_sem=bit_recv.at[i],
            device_id=(g ^ (1 << (bits - 1 - i)), s),
            device_id_type=MESH,
        )

    for i in range(bits):
        bit_copy(i).start()
        bit_copy(i).wait()

    def widen(d, carry):
        spread = blocks * heads
        at = pl.ds(pl.multiple_of(d * spread, spread), spread)
        for kv in range(2):
            spot = d // seqs
            spot = (spot // low, *((spot >> bit) % 2 for bit in reversed(range(bits))), d % seqs)
            wide[kv, at, :] = gathered[(*spot, pl.ds(kv * spread, spread))].astype(jnp.float32)
        return carry

    lax.fori_loop(0, devices, widen, 0)
    loads[4].wait()

    factor = math.log2(math.e) / math.sqrt(HEAD_DIM)
    left_bias = jnp.where(has_left, 0.0, -jnp.inf)
    right_bias = jnp.where(has_right, 0.0, -jnp.inf)

    def attend_head(h, ready):
        cols = columns(h)
        rows_of = pl.ds(h, total_blocks, stride=heads)
        qh, kh, vh = q[:, cols], k[:, cols], v[:, cols]
        sk = wide[0, rows_of, :].astype(jnp.bfloat16)
        sv = wide[1, rows_of, :].astype(jnp.bfloat16)
        s_own = dot_t(qh, kh)
        if blocks > 2:
            gap = (
                lax.broadcasted_iota(jnp.int32, (rows, rows), 0) // BLOCK
                - lax.broadcasted_iota(jnp.int32, (rows, rows), 1) // BLOCK
            )
            s_own = jnp.where(jnp.abs(gap) <= 1, s_own, -jnp.inf)
        s_sum = dot_t(qh, sk) + bias[...]
        ready()
        s_left = dot_t(qh[:BLOCK], halo[0, 0, :, cols]) + left_bias
        s_right = dot_t(qh[rows - BLOCK :], halo[1, 0, :, cols]) + right_bias
        middle = [jnp.full((rows - 2 * BLOCK, BLOCK), -jnp.inf)] if blocks > 2 else []
        s_halo = jnp.concatenate([s_left, *middle, s_right], axis=0)
        peak = jnp.maximum(
            jnp.max(s_sum, axis=-1, keepdims=True),
            jnp.maximum(
                jnp.max(s_own, axis=-1, keepdims=True),
                jnp.max(s_halo, axis=-1, keepdims=True),
            ),
        )
        w_own = jnp.exp2((s_own - peak) * factor)
        w_halo = jnp.exp2((s_halo - peak) * factor)
        w_sum = jnp.exp2((s_sum - peak) * factor)
        total = (
            jnp.sum(w_own, axis=-1, keepdims=True)
            + jnp.sum(w_halo, axis=-1, keepdims=True)
            + jnp.sum(w_sum, axis=-1, keepdims=True)
        )
        r_halo = w_halo.astype(jnp.bfloat16)
        acc = dot(w_own.astype(jnp.bfloat16), vh) + dot(w_sum.astype(jnp.bfloat16), sv)
        vl, vr = halo[0, 1, :, cols], halo[1, 1, :, cols]
        middle = [jnp.zeros((rows - 2 * BLOCK, HEAD_DIM), jnp.float32)] if blocks > 2 else []
        acc = acc + jnp.concatenate(
            [dot(r_halo[:BLOCK], vl), *middle, dot(r_halo[rows - BLOCK :], vr)], axis=0
        )
        out[:, cols] = (acc / total).astype(jnp.bfloat16)

    def arrived(u):
        for side, there in ((0, has_left), (1, has_right)):
            @pl.when(there)
            def _(side=side):
                edge(side, u).wait_recv()

    steps = UNIT_HEADS // STEP_HEADS

    def attend(step, carry):
        u = step // steps

        @pl.when(step % steps == 0)
        def _():
            if relaying:
                @pl.when(far & jnp.logical_not(at_once) & (u < passing))
                def _():
                    pass_on(u)

            arrived(u)

        for i in range(STEP_HEADS):
            attend_head(step * STEP_HEADS + i, lambda: None)
        return carry

    lax.fori_loop(0, units * steps, attend, 0)

    def sent(lo, hi):
        for side in range(2):
            @pl.when(exists(side))
            def _(side=side):
                each(lo, hi, lambda u: edge(side, u).wait_send())

    for i, (lo, n) in enumerate(taper):
        if i + 1 == len(taper):
            sent(0, units)
            if relaying:
                @pl.when(far)
                def _():
                    each(0, passing, lambda u: forward(u).wait_send())

                @pl.when(lead_relay)
                def _():
                    forward(units + LEAD_TAPER).wait_send()

            for step in range(1, planes):
                for way in range(2):
                    @pl.when(line_sends(way, step))
                    def _(way=way, step=step):
                        line_copy(way, step).wait_send()

        for h in range(lo, lo + n):
            attend_head(h, (lambda i=i: arrived(units + i)) if h == lo else lambda: None)

    for side in range(2):
        @pl.when(exists(side))
        def _(side=side):
            for i in range(len(taper)):
                edge(side, units + i).wait_send()


def edge_units(heads):
    units = (heads - sum(TAPER)) // UNIT_HEADS
    lo, taper = units * UNIT_HEADS, []
    for n in (heads - lo - sum(TAPER), *TAPER):
        if n:
            taper.append((lo, n))
            lo += n
    return units, taper


def gather_shape(groups):
    bits = min(groups.bit_length() - 1, PLANE_BITS)
    return bits, groups >> bits


def relays(groups, seqs):
    return seqs == 2 and groups >= 8


def solution(mesh):
    groups, seqs = mesh.shape["grp"], mesh.shape["seq"]
    assert groups & (groups - 1) == 0

    def shards(queries, keys, values, global_pos, layout):
        rows, width = queries.shape
        blocks, heads = rows // BLOCK, width // HEAD_DIM
        devices = groups * seqs
        units, taper = edge_units(heads)
        units += len(taper)
        bits, planes = gather_shape(groups)
        summaries = devices * blocks * width
        limit = 2 * (4 * rows + 6 * BLOCK) * width + 12 * summaries + (8 << 20)
        operands = [
            pltpu.with_memory_space_constraint(a, pltpu.HBM)
            for a in (global_pos, layout, queries, keys, values)
        ]
        return pl.pallas_call(
            functools.partial(kernel, groups, seqs),
            out_shape=pltpu.VMEM((rows, width), jnp.bfloat16),
            in_specs=[pl.BlockSpec(memory_space=pltpu.HBM)] * 5,
            out_specs=pl.BlockSpec(memory_space=pltpu.VMEM),
            scratch_shapes=[
                pltpu.SMEM(global_pos.shape, jnp.int32),
                pltpu.SMEM(layout.shape, jnp.int32),
                pltpu.VMEM((rows, width), jnp.bfloat16),
                pltpu.VMEM((2, rows, width), jnp.bfloat16),
                pltpu.VMEM((2, 2, BLOCK, width), jnp.bfloat16),
                pltpu.VMEM((2, BLOCK, width), jnp.bfloat16),
                pltpu.VMEM((planes, *(2,) * bits, seqs, 2 * blocks * heads, HEAD_DIM), jnp.bfloat16),
                pltpu.VMEM((2 * blocks * heads, HEAD_DIM), jnp.float32),
                pltpu.VMEM((2, devices * blocks * heads, HEAD_DIM), jnp.float32),
                pltpu.VMEM((rows, devices * blocks), jnp.float32),
                pltpu.SemaphoreType.DMA((7,)),
                pltpu.SemaphoreType.DMA((2, units)),
                pltpu.SemaphoreType.DMA((2, units)),
                pltpu.SemaphoreType.DMA((units,)),
                pltpu.SemaphoreType.DMA((units,)),
                pltpu.SemaphoreType.DMA((seqs,)),
                pltpu.SemaphoreType.DMA((seqs,)),
                pltpu.SemaphoreType.DMA((2, planes)),
                pltpu.SemaphoreType.DMA((2, planes)),
                pltpu.SemaphoreType.DMA((max(bits, 1),)),
                pltpu.SemaphoreType.DMA((max(bits, 1),)),
            ],
            compiler_params=pltpu.CompilerParams(
                collective_id=0, has_side_effects=True, vmem_limit_bytes=limit
            ),
        )(*operands)

    both = ("grp", "seq")
    in_specs = (P(both, None), P(both, None), P(both, None), P(both), P(both, None))
    return jax.shard_map(
        shards, mesh=mesh, in_specs=in_specs, out_specs=P(both, None), check_vma=False
    )
```

```python
import functools
import math

import jax
import jax.numpy as jnp
from jax import lax
from jax.experimental import pallas as pl
from jax.experimental.pallas import tpu as pltpu
from jax.sharding import PartitionSpec as P

HEAD_DIM = 128
BLOCK = 128
STEP_HEADS = 2
UNIT_HEADS = 4
TAPER = (2, 1, 1)
EARLY_UNITS = 1
LEAD_UNITS = 1
LEAD_TAPER = 1
SWAP = True
PLANE_BITS = 2
POOL_HEADS = 8
MESH = pl.DeviceIdType.MESH


def dot_t(a, b):
    return lax.dot_general(a, b, (((1,), (1,)), ((), ())), preferred_element_type=jnp.float32)


def dot(a, b):
    return jnp.dot(a, b, preferred_element_type=jnp.float32)


def kernel(
    groups, seqs, pos_hbm, layout_hbm, q_hbm, k_hbm, v_hbm, out,
    pos_ref, layout_ref, q, kv_own, halo, relay, gathered, own, wide, bias,
    load_sem, send_sem, recv_sem, relay_recv, relay_send, seq_send, seq_recv,
    line_send, line_recv, bit_send, bit_recv,
):
    rows, width = q.shape
    k, v = kv_own.at[0], kv_own.at[1]
    heads = width // HEAD_DIM
    blocks = rows // BLOCK
    devices = groups * seqs
    total_blocks = devices * blocks
    bits, planes = gather_shape(groups)
    low = 1 << bits
    relaying = relays(groups, seqs)

    g, s = lax.axis_index("grp"), lax.axis_index("seq")
    me = g * seqs + s
    has_left, has_right = me > 0, me < devices - 1
    plane, lane = g // low, g % low

    def coords(position):
        return (position // seqs, position % seqs)

    first = s % 2
    second = 1 - first

    def exists(side):
        return jnp.where(side == 0, has_right, has_left)

    def neighbour(side):
        return jnp.clip(me + 1 - 2 * side, 0, devices - 1)

    pairs = groups // 2
    step_pair = 2 * seqs
    far = (g % 2 == s) if relaying else False
    rank = jnp.where(s == 0, g // 2, pairs - 1 - g // 2)
    odd = rank % 2 == 1
    across = me + (step_pair - 1) * (1 - 2 * s)
    behind, ahead = me + step_pair * (1 - 2 * s), me - step_pair * (1 - 2 * s)
    handed = jnp.where(far, heads * jnp.where(odd, 1, rank) // (pairs * UNIT_HEADS), 0) if relaying else 0
    via = jnp.where(odd, ahead, across)
    passing = heads * jnp.where(odd, pairs - 1 - rank, 1) // (pairs * UNIT_HEADS)
    target = jnp.where(odd, behind, across)
    target_side = jnp.where(odd, first, second)
    apart = (s == 1) & (g < 2) if relaying else False
    lead, lead_relay = apart & (g == 0), apart & (g == 1)
    hand_side = jnp.where(lead, first, second)
    if relaying:
        handed = jnp.where(lead, LEAD_UNITS, handed)
        via = jnp.where(lead, me + seqs, via)
        passing = jnp.where(lead_relay, LEAD_UNITS, passing)
        target = jnp.where(lead_relay, across, target)
    at_once = jnp.logical_not(odd) | lead_relay

    units, taper = edge_units(heads)
    early = min(EARLY_UNITS, units)
    split = early * UNIT_HEADS * HEAD_DIM
    ahead_cols, rest_cols = pl.ds(0, split), pl.ds(split, width - split)
    moves = [(x.at[:, part], y.at[:, part]) for part in (ahead_cols, rest_cols) for x, y in ((k_hbm, k), (v_hbm, v))]
    moves += [(q_hbm, q), (pos_hbm, pos_ref), (layout_hbm, layout_ref)]
    loads = [pltpu.make_async_copy(x, y, load_sem.at[i]) for i, (x, y) in enumerate(moves)]
    for load in loads[:4]:
        load.start()
    barrier = pltpu.get_barrier_semaphore()

    peers = [(True, g * seqs + lax.rem(s + o, seqs)) for o in range(1, seqs)]
    if seqs == 2:
        peers += [(exists(second), neighbour(second))]
    else:
        peers += [(exists(side), neighbour(side)) for side in range(2)]
    peers += [(True, (g ^ (1 << bit)) * seqs + s) for bit in range(bits)]
    if planes > 1:
        peers += [
            (plane > 0, jnp.maximum(me - low * seqs, 0)),
            (plane < planes - 1, jnp.minimum(me + low * seqs, devices - 1)),
        ]
    if relaying:
        peers += [(far, across), (far & (rank > 0), ahead), (far & (rank < pairs - 1), behind)]
    expected = 0
    for there, peer in peers:
        if there is True:
            pl.semaphore_signal(barrier, inc=1, device_id=coords(peer), device_id_type=MESH)
            expected = expected + 1
        else:
            @pl.when(there)
            def _(peer=peer):
                pl.semaphore_signal(barrier, inc=1, device_id=coords(peer), device_id_type=MESH)
            expected = expected + there.astype(jnp.int32)
    for load in loads[4:]:
        load.start()
    pl.semaphore_wait(barrier, expected)

    def columns(h):
        return pl.ds(pl.multiple_of(h * HEAD_DIM, HEAD_DIM), HEAD_DIM)

    def span(u):
        if isinstance(u, int) and u >= units:
            lo, n = taper[u - units]
            return pl.ds(lo * HEAD_DIM, n * HEAD_DIM)
        return pl.ds(pl.multiple_of(u * UNIT_HEADS * HEAD_DIM, UNIT_HEADS * HEAD_DIM), UNIT_HEADS * HEAD_DIM)

    def edge(side, u):
        start = pl.multiple_of((rows - BLOCK) * (1 - side), BLOCK)
        return pltpu.make_async_remote_copy(
            src_ref=kv_own.at[:, pl.ds(start, BLOCK), span(u)],
            dst_ref=halo.at[side, :, :, span(u)],
            send_sem=send_sem.at[side, u],
            recv_sem=recv_sem.at[side, u],
            device_id=coords(neighbour(side)),
            device_id_type=MESH,
        )

    def hand(u):
        start = pl.multiple_of((rows - BLOCK) * (1 - hand_side), BLOCK)
        return pltpu.make_async_remote_copy(
            src_ref=kv_own.at[:, pl.ds(start, BLOCK), span(u)],
            dst_ref=relay.at[:, :, span(u)],
            send_sem=send_sem.at[hand_side, u],
            recv_sem=relay_recv.at[u],
            device_id=coords(jnp.clip(via, 0, devices - 1)),
            device_id_type=MESH,
        )

    def forward(u):
        return pltpu.make_async_remote_copy(
            src_ref=relay.at[:, :, span(u)],
            dst_ref=halo.at[target_side, :, :, span(u)],
            send_sem=relay_send.at[u],
            recv_sem=recv_sem.at[target_side, u],
            device_id=coords(jnp.clip(target, 0, devices - 1)),
            device_id_type=MESH,
        )

    def pass_on(u):
        hand(u).wait_recv()
        forward(u).start()

    def each(lo, hi, act):
        def body(u, carry):
            act(u)
            return carry

        lax.fori_loop(lo, hi, body, 0)

    def every(lo, act):
        each(lo, units, act)
        for i in range(len(taper)):
            act(units + i)

    def send(sides):
        def act(u):
            for side in sides:
                if not relaying or (isinstance(u, int) and u >= units and u != units + LEAD_TAPER):
                    edge(side, u).start()
                    continue
                stop = (lead if isinstance(u, int) and u >= units else u < handed) & (side == hand_side)

                @pl.when(stop)
                def _():
                    hand(u).start()

                @pl.when(jnp.logical_not(stop))
                def _(side=side):
                    edge(side, u).start()

        return act

    ahead_side = jnp.where((s == 1) & (g % 2 == 0), second, first) if SWAP else first
    both = exists(first) & exists(second) & jnp.logical_not(apart)

    loads[0].wait()
    loads[1].wait()

    @pl.when(both)
    def _():
        each(0, early, send((ahead_side, 1 - ahead_side)))

    @pl.when(exists(first) & jnp.logical_not(both))
    def _():
        each(0, early, send((first,)))

    loads[2].wait()
    loads[3].wait()
    picks = (
        lax.broadcasted_iota(jnp.int32, (16, rows), 1) // BLOCK
        == lax.broadcasted_iota(jnp.int32, (16, rows), 0)
    ).astype(jnp.bfloat16)

    def pool(step, carry):
        for i in range(POOL_HEADS):
            h = step * POOL_HEADS + i
            cols = columns(h)
            for kv, src in enumerate((k, v)):
                mean = dot(picks, src[:, cols])[:8] * (1.0 / BLOCK)
                spread = jnp.mean(mean * mean, axis=-1, keepdims=True)
                scaled = mean / jnp.sqrt(spread + 1e-06)
                for b in range(blocks):
                    own[pl.ds((kv * blocks + b) * heads + h, 1), :] = scaled[b : b + 1]
        return carry

    lax.fori_loop(0, heads // POOL_HEADS, pool, 0)
    digits = [(lane >> bit) % 2 for bit in reversed(range(bits))]
    gathered[(plane, *digits, s)] = own[...].astype(jnp.bfloat16)

    def seq_copy(o):
        mine = gathered.at[(pl.ds(plane, 1), *(pl.ds(d, 1) for d in digits), pl.ds(s, 1))]
        return pltpu.make_async_remote_copy(
            src_ref=mine,
            dst_ref=mine,
            send_sem=seq_send.at[o],
            recv_sem=seq_recv.at[o],
            device_id=(g, lax.rem(s + o, seqs)),
            device_id_type=MESH,
        )

    for o in range(1, seqs):
        seq_copy(o).start()

    if relaying:
        @pl.when(far & at_once)
        def _():
            each(0, passing, pass_on)

        @pl.when(lead_relay)
        def _():
            pass_on(units + LEAD_TAPER)

    @pl.when(both)
    def _():
        every(early, send((ahead_side, 1 - ahead_side)))

    @pl.when(exists(first) & jnp.logical_not(both))
    def _():
        every(early, send((first,)))

    @pl.when(exists(second) & apart)
    def _():
        every(0, send((second,)))

    loads[5].wait()
    loads[6].wait()
    ids = lax.broadcasted_iota(jnp.int32, (BLOCK, total_blocks), 1)
    spots = lax.broadcasted_iota(jnp.int32, (BLOCK, total_blocks), 0)
    for b in range(blocks):
        seen = spots == pos_ref[b]
        for link in range(layout_ref.shape[1]):
            seen = seen | (ids == layout_ref[b, link])
        bias[b * BLOCK : (b + 1) * BLOCK, :] = jnp.where(seen, 0.0, -jnp.inf)

    @pl.when(jnp.logical_not(has_left))
    def _():
        halo[0] = jnp.zeros(halo.shape[1:], halo.dtype)

    @pl.when(jnp.logical_not(has_right))
    def _():
        halo[1] = jnp.zeros(halo.shape[1:], halo.dtype)

    for o in range(1, seqs):
        seq_copy(o).wait()

    def line_copy(way, step):
        there = jnp.clip(plane + 1 - 2 * way, 0, planes - 1)
        part = jnp.clip(plane + (step - 1) * (2 * way - 1), 0, planes - 1)
        part = gathered.at[(pl.ds(part, 1), *(pl.ds(d, 1) for d in digits))]
        return pltpu.make_async_remote_copy(
            src_ref=part,
            dst_ref=part,
            send_sem=line_send.at[way, step],
            recv_sem=line_recv.at[way, step],
            device_id=(there * low + lane, s),
            device_id_type=MESH,
        )

    def line_sends(way, step):
        if way == 0:
            return (plane < planes - 1) & (plane - step + 1 >= 0)
        return (plane > 0) & (plane + step - 1 < planes)

    def line_gets(way, step):
        return plane - step >= 0 if way == 0 else plane + step < planes

    for step in range(1, planes):
        for way in range(2):
            @pl.when(line_sends(way, step))
            def _(way=way, step=step):
                line_copy(way, step).start()
        for way in range(2):
            @pl.when(line_gets(way, step))
            def _(way=way, step=step):
                line_copy(way, step).wait_recv()

    def bit_copy(i):
        part = gathered.at[
            (slice(None), *(slice(None) if n < i else pl.ds(d, 1) for n, d in enumerate(digits)))
        ]
        return pltpu.make_async_remote_copy(
            src_ref=part,
            dst_ref=part,
            send_sem=bit_send.at[i],
            recv_sem=bit_recv.at[i],
            device_id=(g ^ (1 << (bits - 1 - i)), s),
            device_id_type=MESH,
        )

    for i in range(bits):
        bit_copy(i).start()
        bit_copy(i).wait()

    def widen(d, carry):
        spread = blocks * heads
        at = pl.ds(pl.multiple_of(d * spread, spread), spread)
        for kv in range(2):
            spot = d // seqs
            spot = (spot // low, *((spot >> bit) % 2 for bit in reversed(range(bits))), d % seqs)
            wide[kv, at, :] = gathered[(*spot, pl.ds(kv * spread, spread))].astype(jnp.float32)
        return carry

    lax.fori_loop(0, devices, widen, 0)
    loads[4].wait()

    factor = math.log2(math.e) / math.sqrt(HEAD_DIM)
    left_bias = jnp.where(has_left, 0.0, -jnp.inf)
    right_bias = jnp.where(has_right, 0.0, -jnp.inf)

    def attend_head(h, ready):
        cols = columns(h)
        rows_of = pl.ds(h, total_blocks, stride=heads)
        qh, kh, vh = q[:, cols], k[:, cols], v[:, cols]
        sk = wide[0, rows_of, :].astype(jnp.bfloat16)
        sv = wide[1, rows_of, :].astype(jnp.bfloat16)
        s_own = dot_t(qh, kh)
        if blocks > 2:
            gap = (
                lax.broadcasted_iota(jnp.int32, (rows, rows), 0) // BLOCK
                - lax.broadcasted_iota(jnp.int32, (rows, rows), 1) // BLOCK
            )
            s_own = jnp.where(jnp.abs(gap) <= 1, s_own, -jnp.inf)
        s_sum = dot_t(qh, sk) + bias[...]
        ready()
        s_left = dot_t(qh[:BLOCK], halo[0, 0, :, cols]) + left_bias
        s_right = dot_t(qh[rows - BLOCK :], halo[1, 0, :, cols]) + right_bias
        middle = [jnp.full((rows - 2 * BLOCK, BLOCK), -jnp.inf)] if blocks > 2 else []
        s_halo = jnp.concatenate([s_left, *middle, s_right], axis=0)
        peak = jnp.maximum(
            jnp.max(s_sum, axis=-1, keepdims=True),
            jnp.maximum(
                jnp.max(s_own, axis=-1, keepdims=True),
                jnp.max(s_halo, axis=-1, keepdims=True),
            ),
        )
        w_own = jnp.exp2((s_own - peak) * factor)
        w_halo = jnp.exp2((s_halo - peak) * factor)
        w_sum = jnp.exp2((s_sum - peak) * factor)
        total = (
            jnp.sum(w_own, axis=-1, keepdims=True)
            + jnp.sum(w_halo, axis=-1, keepdims=True)
            + jnp.sum(w_sum, axis=-1, keepdims=True)
        )
        r_halo = w_halo.astype(jnp.bfloat16)
        acc = dot(w_own.astype(jnp.bfloat16), vh) + dot(w_sum.astype(jnp.bfloat16), sv)
        vl, vr = halo[0, 1, :, cols], halo[1, 1, :, cols]
        middle = [jnp.zeros((rows - 2 * BLOCK, HEAD_DIM), jnp.float32)] if blocks > 2 else []
        acc = acc + jnp.concatenate(
            [dot(r_halo[:BLOCK], vl), *middle, dot(r_halo[rows - BLOCK :], vr)], axis=0
        )
        out[:, cols] = (acc / total).astype(jnp.bfloat16)

    def arrived(u):
        for side, there in ((0, has_left), (1, has_right)):
            @pl.when(there)
            def _(side=side):
                edge(side, u).wait_recv()

    steps = UNIT_HEADS // STEP_HEADS

    def attend(step, carry):
        u = step // steps

        @pl.when(step % steps == 0)
        def _():
            if relaying:
                @pl.when(far & jnp.logical_not(at_once) & (u < passing))
                def _():
                    pass_on(u)

            arrived(u)

        for i in range(STEP_HEADS):
            attend_head(step * STEP_HEADS + i, lambda: None)
        return carry

    lax.fori_loop(0, units * steps, attend, 0)

    def sent(lo, hi):
        for side in range(2):
            @pl.when(exists(side))
            def _(side=side):
                each(lo, hi, lambda u: edge(side, u).wait_send())

    for i, (lo, n) in enumerate(taper):
        if i + 1 == len(taper):
            sent(0, units)
            if relaying:
                @pl.when(far)
                def _():
                    each(0, passing, lambda u: forward(u).wait_send())

                @pl.when(lead_relay)
                def _():
                    forward(units + LEAD_TAPER).wait_send()

            for step in range(1, planes):
                for way in range(2):
                    @pl.when(line_sends(way, step))
                    def _(way=way, step=step):
                        line_copy(way, step).wait_send()

        for h in range(lo, lo + n):
            attend_head(h, (lambda i=i: arrived(units + i)) if h == lo else lambda: None)

    for side in range(2):
        @pl.when(exists(side))
        def _(side=side):
            for i in range(len(taper)):
                edge(side, units + i).wait_send()


def edge_units(heads):
    units = (heads - sum(TAPER)) // UNIT_HEADS
    lo, taper = units * UNIT_HEADS, []
    for n in (heads - lo - sum(TAPER), *TAPER):
        if n:
            taper.append((lo, n))
            lo += n
    return units, taper


def gather_shape(groups):
    bits = min(groups.bit_length() - 1, PLANE_BITS)
    return bits, groups >> bits


def relays(groups, seqs):
    return seqs == 2 and groups >= 8


def solution(mesh):
    groups, seqs = mesh.shape["grp"], mesh.shape["seq"]
    assert groups & (groups - 1) == 0

    def shards(queries, keys, values, global_pos, layout):
        rows, width = queries.shape
        blocks, heads = rows // BLOCK, width // HEAD_DIM
        devices = groups * seqs
        units, taper = edge_units(heads)
        units += len(taper)
        bits, planes = gather_shape(groups)
        summaries = devices * blocks * width
        limit = 2 * (4 * rows + 6 * BLOCK) * width + 12 * summaries + (8 << 20)
        operands = [
            pltpu.with_memory_space_constraint(a, pltpu.HBM)
            for a in (global_pos, layout, queries, keys, values)
        ]
        return pl.pallas_call(
            functools.partial(kernel, groups, seqs),
            out_shape=pltpu.VMEM((rows, width), jnp.bfloat16),
            in_specs=[pl.BlockSpec(memory_space=pltpu.HBM)] * 5,
            out_specs=pl.BlockSpec(memory_space=pltpu.VMEM),
            scratch_shapes=[
                pltpu.SMEM(global_pos.shape, jnp.int32),
                pltpu.SMEM(layout.shape, jnp.int32),
                pltpu.VMEM((rows, width), jnp.bfloat16),
                pltpu.VMEM((2, rows, width), jnp.bfloat16),
                pltpu.VMEM((2, 2, BLOCK, width), jnp.bfloat16),
                pltpu.VMEM((2, BLOCK, width), jnp.bfloat16),
                pltpu.VMEM((planes, *(2,) * bits, seqs, 2 * blocks * heads, HEAD_DIM), jnp.bfloat16),
                pltpu.VMEM((2 * blocks * heads, HEAD_DIM), jnp.float32),
                pltpu.VMEM((2, devices * blocks * heads, HEAD_DIM), jnp.float32),
                pltpu.VMEM((rows, devices * blocks), jnp.float32),
                pltpu.SemaphoreType.DMA((7,)),
                pltpu.SemaphoreType.DMA((2, units)),
                pltpu.SemaphoreType.DMA((2, units)),
                pltpu.SemaphoreType.DMA((units,)),
                pltpu.SemaphoreType.DMA((units,)),
                pltpu.SemaphoreType.DMA((seqs,)),
                pltpu.SemaphoreType.DMA((seqs,)),
                pltpu.SemaphoreType.DMA((2, planes)),
                pltpu.SemaphoreType.DMA((2, planes)),
                pltpu.SemaphoreType.DMA((max(bits, 1),)),
                pltpu.SemaphoreType.DMA((max(bits, 1),)),
            ],
            compiler_params=pltpu.CompilerParams(
                collective_id=0, has_side_effects=True, vmem_limit_bytes=limit
            ),
        )(*operands)

    both = ("grp", "seq")
    in_specs = (P(both, None), P(both, None), P(both, None), P(both), P(both, None))
    return jax.shard_map(
        shards, mesh=mesh, in_specs=in_specs, out_specs=P(both, None), check_vma=False
    )
```
